8 devices in a mesh: stage: 4 (over z, y, x), tp: 2 (over core).
Axes of the slice: x: 2, y: 2, z: 1, core: 2. Of those that a mesh axis runs over, the one named last changes fastest.
Arguments:
- x: bfloat16 [4, 4096, 1536], P(None, 'tp')
- g: bfloat16 [4, 2, 1536], P('stage')
- w1: bfloat16 [4, 2, 1536, 6144], P('stage', None, None, 'tp')
- w2: bfloat16 [4, 2, 6144, 1536], P('stage', None, 'tp')
Outputs:
- output: bfloat16 [4, 4, 4096, 1536], P('stage', None, 'tp')
All inputs are finite; a program needn't handle non-finite values.
Results may differ from the reference program's by a relative error of at most 0.0197235.
Values are sent between devices in bfloat16 or wider.
A program may use at most 1 GiB of HBM per device.

```python
import jax
import jax.numpy as jnp
from jax import lax

STAGES = 4
BLOCKS = 2
M = 4
T = 4096
D = 1536
FF = 6144

EPS = 1e-5


def setup_inputs(seed: int = 0) -> dict:
    k = jax.random.split(jax.random.key(seed), 4)
    x = jax.random.normal(k[0], (M, T, D), jnp.float32)
    g = 1.0 + 0.2 * jax.random.normal(k[1], (STAGES, BLOCKS, D), jnp.float32)
    w1 = jax.random.normal(k[2], (STAGES, BLOCKS, D, FF), jnp.float32) * D ** -0.5
    w2 = jax.random.normal(k[3], (STAGES, BLOCKS, FF, D), jnp.float32) * FF ** -0.5
    return {'x': x.astype(jnp.bfloat16), 'g': g.astype(jnp.bfloat16),
            'w1': w1.astype(jnp.bfloat16), 'w2': w2.astype(jnp.bfloat16)}


def _block(y, g, w1, w2):
    yf = y.astype(jnp.float32)
    mu = jnp.mean(yf, axis=-1, keepdims=True)
    var = jnp.mean(jnp.square(yf - mu), axis=-1, keepdims=True)
    h = ((yf - mu) * lax.rsqrt(var + EPS) * g.astype(jnp.float32)).astype(jnp.bfloat16)
    a = jax.nn.gelu(jnp.dot(h, w1, preferred_element_type=jnp.float32)).astype(jnp.bfloat16)
    return (yf + jnp.dot(a, w2, preferred_element_type=jnp.float32)).astype(jnp.bfloat16)


def reference(x, g, w1, w2):
    def one(xm):
        y = xm
        outs = []
        for s in range(STAGES):
            for b in range(BLOCKS):
                y = _block(y, g[s, b], w1[s, b], w2[s, b])
            outs.append(y)
        return jnp.stack(outs)
    return jnp.transpose(lax.map(one, x), (1, 0, 2, 3))
```

```python
import functools

import jax
import jax.numpy as jnp
from jax import lax
from jax.experimental import pallas as pl
from jax.experimental.pallas import tpu as pltpu
from jax.sharding import PartitionSpec as P

EPS = 1e-5
EXPLICIT = False
C = 128
NS = 8
NO = 4
F1K = 18
T = 256


def _gelu(u):
    k0 = 0.7978845608028654
    k1 = k0 * 0.044715
    return u * (0.5 + 0.5 * jnp.tanh(u * (k0 + k1 * (u * u))))


def _kernel(S, M, TL, D, FH, x, g, w1, w2, y,
            w1v, w2v, gv, gf, ybuf, ob, h, a,
            rs, ss, osem, yr, xs, wl, wrs, wrr, gs, credit):
    KT, NH = D // T, FH // T
    NT = 2 * NH
    NP, N2 = NT // 2, KT // 2
    CPM = TL // C
    HC = M * CPM
    NC = 2 * HC
    LX = NS - 2

    p = lax.axis_index('stage')
    i = lax.axis_index('tp')
    j = 2 * p + i
    last = 2 * S - 1
    has_prev, has_next = j > 0, j < last
    odd = i == 1
    prv = (lax.rem(p + S - 1 + i, S), 1 - i)
    nxt = (lax.rem(p + i, S), 1 - i)
    partner = (p, 1 - i)
    MESH = pl.DeviceIdType.MESH

    def tok(ref, q):
        q = lax.rem(q, HC)
        return ref.at[lax.div(q, CPM), pl.ds(pl.multiple_of(lax.rem(q, CPM) * C, C), C), :]

    def arrival(q):
        s = lax.rem(q, NS)
        return pltpu.make_async_copy(tok(x, q), ybuf.at[s], rs.at[s])

    def send(q):
        so, s = lax.rem(q, NO), lax.rem(q, NS)
        return pltpu.make_async_remote_copy(ob.at[so], ybuf.at[s], ss.at[so], rs.at[s], device_id=nxt, device_id_type=MESH)

    def out_local(q):
        so = lax.rem(q, NO)
        return pltpu.make_async_copy(ob.at[so], tok(y.at[0], q), osem.at[so])

    def out_remote(q):
        so = lax.rem(q, NO)
        return pltpu.make_async_remote_copy(ob.at[so], tok(y.at[0], q), osem.at[so], yr.at[0], device_id=partner, device_id_type=MESH)

    def xpush(q):
        s = lax.rem(q, NS)
        return pltpu.make_async_remote_copy(tok(x, q), ybuf.at[s], xs.at[0], rs.at[s], device_id=prv, device_id_type=MESH)

    local1 = [pltpu.make_async_copy(w1.at[0, i, :, pl.ds(n * T, T)], w1v.at[n], wl.at[0]) for n in range(NH)]
    local2 = [pltpu.make_async_copy(w2.at[0, i, :, pl.ds(n * T, T)], w2v.at[n, pl.ds(0, FH), :], wl.at[1]) for n in range(KT)]
    remote1 = [pltpu.make_async_remote_copy(w1.at[0, 1 - i, :, pl.ds(n * T, T)], w1v.at[NH + n], wrs.at[0], wrr.at[0],
                                            device_id=partner, device_id_type=MESH) for n in range(NH)]
    remote2 = [pltpu.make_async_remote_copy(w2.at[0, 1 - i, :, pl.ds(n * T, T)], w2v.at[n, pl.ds(FH, FH), :], wrs.at[1], wrr.at[1],
                                            device_id=partner, device_id_type=MESH) for n in range(KT)]
    whole1, whole2 = w1v.at[pl.ds(0, NH)], w2v.at[:, pl.ds(0, FH), :]
    own1, got1, sent1 = (pltpu.make_async_copy(whole1, whole1, sem) for sem in (wl.at[0], wrr.at[0], wrs.at[0]))
    own2, got2, sent2 = (pltpu.make_async_copy(whole2, whole2, sem) for sem in (wl.at[1], wrr.at[1], wrs.at[1]))
    gcopy = pltpu.make_async_copy(g.at[0], gv, gs.at[0])

    bar = pltpu.get_barrier_semaphore()

    @pl.when(has_prev)
    def _():
        pl.semaphore_signal(bar, 1, device_id=prv, device_id_type=MESH)

    @pl.when(has_next)
    def _():
        pl.semaphore_signal(bar, 1, device_id=nxt, device_id_type=MESH)

    gcopy.start()

    @pl.when(j == 0)
    def _():
        for q in range(NS - 1):
            arrival(q).start()

    for cp in local1:
        cp.start()

    @pl.when(has_prev & has_next)
    def _():
        pl.semaphore_wait(bar, 2)

    @pl.when((j == 0) | (j == last))
    def _():
        pl.semaphore_wait(bar, 1)

    for cp in remote1:
        cp.start()
    for cp in local2:
        cp.start()
    for cp in remote2:
        cp.start()

    @pl.when(has_prev)
    def _():
        pl.semaphore_signal(credit, NS, device_id=prv, device_id_type=MESH)

    gcopy.wait()
    gf[...] = jnp.where(odd, gv[1:2, :].astype(jnp.float32), gv[0:1, :].astype(jnp.float32))

    def ln(s):
        for r in range(0, C, 64):
            yf = ybuf[s, r:r + 64, :].astype(jnp.float32)
            mu = jnp.mean(yf, axis=-1, keepdims=True)
            d = yf - mu
            var = jnp.mean(jnp.square(d), axis=-1, keepdims=True)
            hh = (d * lax.rsqrt(var + EPS) * gf[...]).astype(jnp.bfloat16)
            for k in range(KT):
                h[k, r:r + 64, :] = hh[:, k * T:(k + 1) * T]

    def take_in(q):
        arrival(q + 1).wait()

    def slot_free(q):
        @pl.when(has_next)
        def _():
            send(q).wait_send()

        @pl.when(odd)
        def _():
            out_local(q).wait()

    def put_out(q):
        @pl.when(has_next)
        def _():
            pl.semaphore_wait(credit, 1)
            send(q).start()

        @pl.when(odd & (q < HC))
        def _():
            out_remote(q).start()

        @pl.when(odd & (q >= HC))
        def _():
            out_local(q).start()

        @pl.when(has_prev)
        def _():
            pl.semaphore_signal(credit, 1, device_id=prv, device_id_type=MESH)

        @pl.when((j == 0) & (q + NS - 1 < HC))
        def _():
            arrival(q + NS - 1).start()

        @pl.when((j == 1) & (q + LX >= HC) & (q + LX < NC))
        def _():
            @pl.when(q + LX > HC)
            def _():
                xpush(q + LX - 1).wait_send()
            xpush(q + LX).start()

    items2 = [(2, k, n) for k in range(NT) for n in range(N2)]
    items1 = [(1, k, n) for n in range(NP) for k in range(KT)]

    def res_store(q, col, t):
        s, so = lax.rem(q, NS), lax.rem(q, NO)
        ob[so, :, col:col + T] = (ybuf[s, :, col:col + T].astype(jnp.float32) + t).astype(jnp.bfloat16)

    def main(*accs):
        A = (accs[:8], accs[8:])
        acc1 = lambda n: N2 + n % (8 - N2)

        def push(it, reg):
            ty, k, n = it
            for u in range(2):
                w = (w1v if ty == 1 else w2v)[2 * n + u, k * T:(k + 1) * T, :]
                pltpu.matmul_push_rhs(w, staging_register=reg, mxu_index=u)

        def acc(it, reg):
            ty, k, n = it
            lhs = (h if ty == 1 else a)[k]
            for u in range(2):
                pltpu.matmul_acc_lhs(A[u][acc1(n) if ty == 1 else n], lhs, load_staged_rhs=reg)

        def pop1(n):
            if EXPLICIT:
                t = [pltpu.matmul_pop(A[u][acc1(n)]) for u in range(2)]
            else:
                lhs = jnp.concatenate([h[k] for k in range(KT)], axis=1)
                rhs = jnp.concatenate([w1v[2 * n], w1v[2 * n + 1]], axis=1)
                t = jnp.dot(lhs, rhs, preferred_element_type=jnp.float32)
                t = [t[:, :T], t[:, T:]]
            for u in range(2):
                a[2 * n + u] = _gelu(t[u]).astype(jnp.bfloat16)

        def pop2(q, n):
            if EXPLICIT:
                t = [pltpu.matmul_pop(A[u][n]) for u in range(2)]
            else:
                lhs = jnp.concatenate([a[k] for k in range(NT)], axis=1)
                rhs = jnp.concatenate([w2v[2 * n], w2v[2 * n + 1]], axis=1)
                t = jnp.dot(lhs, rhs, preferred_element_type=jnp.float32)
                t = [t[:, :T], t[:, T:]]
            for u in range(2):
                res_store(q, (2 * n + u) * T, t[u])

        def run(items, reg0, hooks, following):
            for idx, it in enumerate(items):
                reg = (reg0 + idx) % 2
                nx = items[idx + 1] if idx + 1 < len(items) else following
                if EXPLICIT:
                    if nx is not None:
                        push(nx, 1 - reg)
                    acc(it, reg)
                if idx in hooks:
                    hooks[idx]()

        L2, L1 = len(items2), len(items1)

        arrival(0).wait()
        ln(0)
        own1.wait()
        hooks = {}
        for n in range(NP - 1):
            hooks[(n + 2) * KT - 1] = functools.partial(pop1, n)

        half = NP // 2
        hooks[half * KT - 2] = got1.wait
        hooks[L1 - 2] = lambda: (own2.wait(), got2.wait())
        if EXPLICIT:
            push(items1[0], 0)
        run(items1, 0, hooks, items2[0])

        def body(q, _):
            def f1():
                take_in(q)

                @pl.when(q >= NO)
                def _():
                    slot_free(q - NO)
                ln(lax.rem(q + 1, NS))

            def f2():
                for n in range(N2):
                    pop2(q, n)
                put_out(q)
            hk = {N2 * 4 - 1: functools.partial(pop1, NP - 1), F1K * N2 - 1: f1, L2 + KT - 1: f2}
            for n in range(NP - 1):
                hk[L2 + (n + 2) * KT - 1] = functools.partial(pop1, n)
            run(items2 + items1, 0, hk, items2[0])
            return 0

        lax.fori_loop(0, NC - 1, body, 0)

        q = jnp.int32(NC - 1)
        slot_free(q - NO)
        run(items2, 0, {N2 * 4 - 1: functools.partial(pop1, NP - 1)}, None)
        for n in range(N2):
            pop2(q, n)
        put_out(q)

    if EXPLICIT:
        pl.run_scoped(main, *([pltpu.ACC(0)((C, T), jnp.float32)] * 8 + [pltpu.ACC(1)((C, T), jnp.float32)] * 8))
    else:
        main(*([None] * 16))

    for d in range(NO):
        slot_free(jnp.int32(NC - NO + d))

    @pl.when(has_next)
    def _():
        pl.semaphore_wait(credit, NS)

    @pl.when(j == 1)
    def _():
        xpush(jnp.int32(NC - 1)).wait_send()

    sent1.wait()
    sent2.wait()

    @pl.when(i == 0)
    def _():
        pltpu.make_async_copy(y, y, yr.at[0]).wait()


def solution(mesh):
    S = mesh.shape['stage']

    def local(x, g, w1, w2):
        M, TL, D = x.shape
        FH = w1.shape[-1]
        bf = jnp.bfloat16
        dma = pltpu.SemaphoreType.DMA
        flops = 4 * M * 2 * TL * D * 2 * FH
        return pl.pallas_call(
            functools.partial(_kernel, S, M, TL, D, FH),
            out_shape=jax.ShapeDtypeStruct((1, M, TL, D), bf),
            in_specs=[pl.BlockSpec(memory_space=pl.ANY)] * 4,
            out_specs=pl.BlockSpec(memory_space=pl.ANY),
            scratch_shapes=[
                pltpu.VMEM((2 * FH // T, D, T), bf),
                pltpu.VMEM((D // T, 2 * FH, T), bf),
                pltpu.VMEM((2, D), bf),
                pltpu.VMEM((1, D), jnp.float32),
                pltpu.VMEM((NS, C, D), bf),
                pltpu.VMEM((NO, C, D), bf),
                pltpu.VMEM((D // T, C, T), bf),
                pltpu.VMEM((2 * FH // T, C, T), bf),
                dma((NS,)), dma((NO,)), dma((NO,)), dma((1,)), dma((1,)),
                dma((2,)), dma((2,)), dma((2,)), dma((1,)),
                pltpu.SemaphoreType.REGULAR,
            ],
            compiler_params=pltpu.CompilerParams(
                collective_id=0, has_side_effects=True, vmem_limit_bytes=67043328),
            cost_estimate=pl.CostEstimate(flops=flops, bytes_accessed=4 * M * TL * D, transcendentals=0),
        )(x, g, w1, w2)

    return jax.shard_map(
        local, mesh=mesh,
        in_specs=(P(None, 'tp', None), P('stage', None, None),
                  P('stage', None, None, 'tp'), P('stage', None, 'tp', None)),
        out_specs=P('stage', None, 'tp', None), check_vma=False)
```

```python
import functools

import jax
import jax.numpy as jnp
from jax import lax
from jax.experimental import pallas as pl
from jax.experimental.pallas import tpu as pltpu
from jax.sharding import PartitionSpec as P

EPS = 1e-5
C = 144
NS = 8
NO = 4
T = 256


def _gelu(u):
    k0 = 0.7978845608028654
    k1 = k0 * 0.044715
    return u * (0.5 + 0.5 * jnp.tanh(u * (k0 + k1 * (u * u))))


def _kernel(S, R, D, FH, x, g, w1, w2, y,
            w1v, w2v, gv, gf, ybuf, ob, h, a,
            rs, ss, osem, otail, yr, xs, wl, wrs, wrr, gs, credit):
    KT, NH = D // T, FH // T
    NT = 2 * NH
    NP, N2 = NT // 2, KT // 2
    HC = -(-R // C)
    OV = HC * C - R
    NC = 2 * HC
    LX = NS - 2
    B = C - OV

    p = lax.axis_index('stage')
    i = lax.axis_index('tp')
    j = 2 * p + i
    last = 2 * S - 1
    has_next = j < last
    odd = i == 1
    prv = (lax.rem(p + S - 1 + i, S), 1 - i)
    nxt = (lax.rem(p + i, S), 1 - i)
    partner = (p, 1 - i)
    MESH = pl.DeviceIdType.MESH

    def rows(q, skip=0, n=C):
        r = lax.rem(q, HC)
        at = r * C - lax.div(r, HC - 1) * OV + skip
        return pl.ds(pl.multiple_of(at, 16), n)

    def arrival(q):
        s = lax.rem(q, NS)
        return pltpu.make_async_copy(x.at[rows(q), :], ybuf.at[s], rs.at[s])

    def send(q):
        so, s = lax.rem(q, NO), lax.rem(q, NS)
        return pltpu.make_async_remote_copy(ob.at[so], ybuf.at[s], ss.at[so], rs.at[s], device_id=nxt, device_id_type=MESH)

    def xpush(q):
        s = lax.rem(q, NS)
        return pltpu.make_async_remote_copy(x.at[rows(q), :], ybuf.at[s], xs.at[0], rs.at[s], device_id=prv, device_id_type=MESH)

    def out_local(q):
        so = lax.rem(q, NO)
        return pltpu.make_async_copy(ob.at[so, pl.ds(OV, B)], y.at[rows(q, OV, B), :], osem.at[so])

    def out_remote(q):
        so = lax.rem(q, NO)
        return pltpu.make_async_remote_copy(ob.at[so, pl.ds(OV, B)], y.at[rows(q, OV, B), :], osem.at[so], yr.at[0],
                                            device_id=partner, device_id_type=MESH)

    def tail_local(q):
        so = lax.rem(q, NO)
        return pltpu.make_async_copy(ob.at[so, pl.ds(0, OV)], y.at[rows(q, 0, OV), :], otail.at[so])

    def tail_remote(q):
        so = lax.rem(q, NO)
        return pltpu.make_async_remote_copy(ob.at[so, pl.ds(0, OV)], y.at[rows(q, 0, OV), :], otail.at[so], yr.at[0],
                                            device_id=partner, device_id_type=MESH)

    def whole(q):
        return lax.rem(q, HC) < HC - 1

    local1 = [pltpu.make_async_copy(w1.at[0, i, :, pl.ds(n * T, T)], w1v.at[n], wl.at[0]) for n in range(NH)]
    local2 = [pltpu.make_async_copy(w2.at[0, i, :, pl.ds(n * T, T)], w2v.at[n, pl.ds(0, FH), :], wl.at[1]) for n in range(KT)]
    remote1 = [pltpu.make_async_remote_copy(w1.at[0, 1 - i, :, pl.ds(n * T, T)], w1v.at[NH + n], wrs.at[0], wrr.at[0],
                                            device_id=partner, device_id_type=MESH) for n in range(NH)]
    remote2 = [pltpu.make_async_remote_copy(w2.at[0, 1 - i, :, pl.ds(n * T, T)], w2v.at[n, pl.ds(FH, FH), :], wrs.at[1], wrr.at[1],
                                            device_id=partner, device_id_type=MESH) for n in range(KT)]
    half1, half2 = w1v.at[pl.ds(0, NH)], w2v.at[:, pl.ds(0, FH), :]
    own1, got1, sent1 = (pltpu.make_async_copy(half1, half1, sem) for sem in (wl.at[0], wrr.at[0], wrs.at[0]))
    own2, got2, sent2 = (pltpu.make_async_copy(half2, half2, sem) for sem in (wl.at[1], wrr.at[1], wrs.at[1]))
    gcopy = pltpu.make_async_copy(g.at[0], gv, gs.at[0])

    bar = pltpu.get_barrier_semaphore()

    pl.semaphore_signal(bar, 1, device_id=prv, device_id_type=MESH)
    pl.semaphore_signal(bar, 1, device_id=nxt, device_id_type=MESH)
    gcopy.start()

    @pl.when(j == 0)
    def _():
        for q in range(NS - 1):
            arrival(q).start()

    for cp in local1:
        cp.start()

    pl.semaphore_wait(bar, 2)
    for cp in remote1:
        cp.start()
    for cp in local2:
        cp.start()
    for cp in remote2:
        cp.start()

    pl.semaphore_signal(credit, NS, device_id=prv, device_id_type=MESH)

    gcopy.wait()
    gf[...] = jnp.where(odd, gv[1:2, :].astype(jnp.float32), gv[0:1, :].astype(jnp.float32))

    def ln(s):
        for r in range(0, C, 48):
            yf = ybuf[s, r:r + 48, :].astype(jnp.float32)
            mu = jnp.mean(yf, axis=-1, keepdims=True)
            d = yf - mu
            var = jnp.mean(jnp.square(d), axis=-1, keepdims=True)
            hh = (d * lax.rsqrt(var + EPS) * gf[...]).astype(jnp.bfloat16)
            for k in range(KT):
                h[k, r:r + 48, :] = hh[:, k * T:(k + 1) * T]

    def mm1(n):
        lhs = jnp.concatenate([h[k] for k in range(KT)], axis=1)
        rhs = jnp.concatenate([w1v[2 * n], w1v[2 * n + 1]], axis=1)
        t = jnp.dot(lhs, rhs, preferred_element_type=jnp.float32)
        for u in range(2):
            a[2 * n + u] = _gelu(t[:, u * T:(u + 1) * T]).astype(jnp.bfloat16)

    def mm2(n, q):
        s, so = lax.rem(q, NS), lax.rem(q, NO)
        lhs = jnp.concatenate([a[k] for k in range(NT)], axis=1)
        rhs = jnp.concatenate([w2v[2 * n], w2v[2 * n + 1]], axis=1)
        t = jnp.dot(lhs, rhs, preferred_element_type=jnp.float32)
        cols = slice(2 * n * T, 2 * (n + 1) * T)
        ob[so, :, cols] = (ybuf[s, :, cols].astype(jnp.float32) + t).astype(jnp.bfloat16)

    def slot_free(q):
        @pl.when(has_next)
        def _():
            send(q).wait_send()

        @pl.when(odd)
        def _():
            out_local(q).wait()

        if OV:
            @pl.when(odd & whole(q))
            def _():
                tail_local(q).wait()

    def put_out(q):
        pl.semaphore_wait(credit, 1)
        pl.semaphore_signal(credit, 1, device_id=prv, device_id_type=MESH)

        @pl.when(has_next)
        def _():
            send(q).start()

        @pl.when(odd & (q < HC))
        def _():
            out_remote(q).start()

        @pl.when(odd & (q >= HC))
        def _():
            out_local(q).start()

        if OV:
            @pl.when(odd & (q < HC) & whole(q))
            def _():
                tail_remote(q).start()

            @pl.when(odd & (q >= HC) & whole(q))
            def _():
                tail_local(q).start()

        @pl.when((j == 0) & (q + NS - 1 < HC))
        def _():
            arrival(q + NS - 1).start()

        @pl.when((j == 1) & (q + LX > HC) & (q + LX < NC))
        def _():
            xpush(q + LX - 1).wait_send()

        @pl.when((j == 1) & (q + LX >= HC) & (q + LX < NC))
        def _():
            xpush(q + LX).start()

    arrival(0).wait()
    ln(0)

    def body(q, first):
        for n in range(NP):
            if first and n == 0:
                own1.wait()
            if first and n == NP // 2:
                got1.wait()
            mm1(n)
        if first:
            own2.wait()
            got2.wait()
        for n in range(N2 - 1):
            mm2(n, q)

        @pl.when(q + 1 < NC)
        def _():
            arrival(q + 1).wait()
        ln(lax.rem(q + 1, NS))
        mm2(N2 - 1, q)
        put_out(q)

        @pl.when(q + 1 >= NO)
        def _():
            slot_free(q + 1 - NO)
        return 0

    body(jnp.int32(0), True)
    lax.fori_loop(1, NC, lambda q, _: body(q, False), 0)

    for d in range(1, NO):
        slot_free(jnp.int32(NC - NO + d))

    pl.semaphore_wait(credit, NS)

    @pl.when(j == 1)
    def _():
        xpush(jnp.int32(NC - 1)).wait_send()

    sent1.wait()
    sent2.wait()

    @pl.when(i == 0)
    def _():
        pltpu.make_async_copy(y, y, yr.at[0]).wait()


def solution(mesh):
    S = mesh.shape['stage']

    def local(x, g, w1, w2):
        M, TL, D = x.shape
        FH = w1.shape[-1]
        bf = jnp.bfloat16
        dma = pltpu.SemaphoreType.DMA
        out = pl.pallas_call(
            functools.partial(_kernel, S, M * TL, D, FH),
            out_shape=jax.ShapeDtypeStruct((M * TL, D), bf),
            in_specs=[pl.BlockSpec(memory_space=pl.ANY)] * 4,
            out_specs=pl.BlockSpec(memory_space=pl.ANY),
            scratch_shapes=[
                pltpu.VMEM((2 * FH // T, D, T), bf),
                pltpu.VMEM((D // T, 2 * FH, T), bf),
                pltpu.VMEM((2, D), bf),
                pltpu.VMEM((1, D), jnp.float32),
                pltpu.VMEM((NS, C, D), bf),
                pltpu.VMEM((NO, C, D), bf),
                pltpu.VMEM((D // T, C, T), bf),
                pltpu.VMEM((2 * FH // T, C, T), bf),
                dma((NS,)), dma((NO,)), dma((NO,)), dma((NO,)), dma((1,)), dma((1,)),
                dma((2,)), dma((2,)), dma((2,)), dma((1,)),
                pltpu.SemaphoreType.REGULAR,
            ],
            compiler_params=pltpu.CompilerParams(
                collective_id=0, has_side_effects=True, vmem_limit_bytes=67043328),
            cost_estimate=pl.CostEstimate(flops=8 * M * TL * D * 2 * FH, bytes_accessed=4 * M * TL * D, transcendentals=0),
        )(x.reshape(M * TL, D), g, w1, w2)
        return out.reshape(1, M, TL, D)

    return jax.shard_map(
        local, mesh=mesh,
        in_specs=(P(None, 'tp', None), P('stage', None, None),
                  P('stage', None, None, 'tp'), P('stage', None, 'tp', None)),
        out_specs=P('stage', None, 'tp', None), check_vma=False)
```

```python
import functools

import jax
import jax.numpy as jnp
from jax import lax
from jax.experimental import pallas as pl
from jax.experimental.pallas import tpu as pltpu
from jax.sharding import PartitionSpec as P

EPS = 1e-5
C = 144
NS = 4
NO = 3
TP = 4
LR = 64 if C % 64 == 0 else 48
T = 256
EARLY = 2


def _gelu(u):
    k0 = 0.7978845608028654
    k1 = k0 * 0.044715
    return u * (0.5 + 0.5 * jnp.tanh(u * (k0 + k1 * (u * u))))


def _kernel(S, R, D, FH, x, g, w1, w2, y,
            w1v, w2v, gv, gf, ybuf, ob, h, a, pb, pr,
            rs, ss, osem, otail, yr, xs, wl, wrs, wrr, gs, ps, prs, credit, pair, seen):
    KT, NH = D // T, FH // T
    NT = 2 * NH
    NP, N2 = NT // 2, KT // 2
    NV, W = w1v.shape[1], w1v.shape[3]
    HC = -(-R // C)
    OV = HC * C - R
    NC = 2 * HC
    LX = NS
    B = C - OV

    p = lax.axis_index('stage')
    i = lax.axis_index('tp')
    j = 2 * p + i
    last = 2 * S - 1
    has_next = j < last
    odd = i == 1
    prv = (lax.rem(p + S - 1 + i, S), 1 - i)
    nxt = (lax.rem(p + i, S), 1 - i)
    partner = (p, 1 - i)
    MESH = pl.DeviceIdType.MESH

    def rows(q, skip=0, n=C):
        r = lax.rem(q, HC)
        at = r * C - lax.div(r, HC - 1) * OV + skip
        return pl.ds(pl.multiple_of(at, 16), n)

    def arrival(q):
        s = lax.rem(q, NS)
        return pltpu.make_async_copy(x.at[rows(q), :], ybuf.at[s], rs.at[s])

    def send(q):
        so, s = lax.rem(q, NO), lax.rem(q, NS)
        return pltpu.make_async_remote_copy(ob.at[so], ybuf.at[s], ss.at[so], rs.at[s], device_id=nxt, device_id_type=MESH)

    def xpush(q):
        s = lax.rem(q, NS)
        return pltpu.make_async_remote_copy(x.at[rows(q), :], ybuf.at[s], xs.at[0], rs.at[s], device_id=prv, device_id_type=MESH)

    def xfeed(q):
        return pltpu.make_async_remote_copy(x.at[rows(q), :], ybuf.at[q], xs.at[0], rs.at[q], device_id=nxt, device_id_type=MESH)

    def out_local(q):
        so = lax.rem(q, NO)
        return pltpu.make_async_copy(ob.at[so, pl.ds(OV, B)], y.at[rows(q, OV, B), :], osem.at[so])

    def out_remote(q):
        so = lax.rem(q, NO)
        return pltpu.make_async_remote_copy(ob.at[so, pl.ds(OV, B)], y.at[rows(q, OV, B), :], osem.at[so], yr.at[0],
                                            device_id=partner, device_id_type=MESH)

    def tail_local(q):
        so = lax.rem(q, NO)
        return pltpu.make_async_copy(ob.at[so, pl.ds(0, OV)], y.at[rows(q, 0, OV), :], otail.at[so])

    def tail_remote(q):
        so = lax.rem(q, NO)
        return pltpu.make_async_remote_copy(ob.at[so, pl.ds(0, OV)], y.at[rows(q, 0, OV), :], otail.at[so], yr.at[0],
                                            device_id=partner, device_id_type=MESH)

    def whole(q):
        return lax.rem(q, HC) < HC - 1

    def base(b):
        return 2 * lax.rem(b + i, 2)

    def deep(third):
        return pl.ds(pl.multiple_of(third * FH, T), FH)

    def load1(b):
        return [pltpu.make_async_copy(w1.at[0, b, :, pl.ds(v * W, W)], w1v.at[base(b), v], wl.at[b]) for v in range(NV)]

    def load2(b):
        return [pltpu.make_async_copy(w2.at[0, b], w2v.at[deep(base(b)), :], wl.at[2 + b])]

    D4, F4 = D // (4 // NV), FH // 4

    def give1(t):
        at = lax.rem(t, 4 // NV), lax.div(t, 4 // NV)
        r, v = pl.ds(pl.multiple_of(at[0] * D4, 16), D4), at[1]
        return pltpu.make_async_remote_copy(w1.at[0, 1 - i, r, pl.ds(pl.multiple_of(v * W, T), W)], w1v.at[1, v, r, :],
                                            wrs.at[0], wrr.at[0], device_id=partner, device_id_type=MESH)

    def give2(t):
        r = lax.rem(t, 4) * F4
        return pltpu.make_async_remote_copy(w2.at[0, 1 - i, pl.ds(pl.multiple_of(r, 16), F4), :],
                                            w2v.at[pl.ds(pl.multiple_of(FH + r, 16), F4), :],
                                            wrs.at[1], wrr.at[1], device_id=partner, device_id_type=MESH)

    half1, half2 = w1v.at[1], w2v.at[pl.ds(0, FH), :]
    got1, sent1 = (pltpu.make_async_copy(half1, half1, sem) for sem in (wrr.at[0], wrs.at[0]))
    got2, sent2 = (pltpu.make_async_copy(half2, half2, sem) for sem in (wrr.at[1], wrs.at[1]))

    def own1(b):
        pltpu.make_async_copy(half1, half1, wl.at[b]).wait()

    def own2(b):
        pltpu.make_async_copy(half2, half2, wl.at[2 + b]).wait()

    def own(b):
        own1(b)
        own2(b)

    def cols1(third, n):
        v, at = divmod(2 * n * T, W)
        return w1v[third, v, :, at:at + 2 * T]

    gcopy = pltpu.make_async_copy(g.at[0], gv, gs.at[0])

    bar = pltpu.get_barrier_semaphore()

    pl.semaphore_signal(bar, 1, device_id=prv, device_id_type=MESH)
    pl.semaphore_signal(bar, 1, device_id=nxt, device_id_type=MESH)
    gcopy.start()

    @pl.when(j == 0)
    def _():
        for q in range(LX):
            arrival(q).start()

    for b in range(2):
        @pl.when((p == 0) | (i == b))
        def _():
            for cp in load1(b) + load2(b):
                cp.start()

    pl.semaphore_wait(bar, 2)
    @pl.when(j == 0)
    def _():
        for q in range(TP):
            xfeed(q).start()

    for t in range(EARLY):
        give1(jnp.int32(t)).start()

    @pl.when(p > 0)
    def _():
        for t in range(EARLY, 4):
            give1(jnp.int32(t)).start()
        for t in range(4):
            give2(jnp.int32(t)).start()

    pl.semaphore_signal(credit, NS, device_id=prv, device_id_type=MESH)

    gcopy.wait()
    for b in range(2):
        gf[b] = gv[b:b + 1, :].astype(jnp.float32)

    def ln(s, b):
        for r in range(0, C, LR):
            yf = ybuf[s, r:r + LR, :].astype(jnp.float32)
            mu = jnp.mean(yf, axis=-1, keepdims=True)
            d = yf - mu
            var = jnp.mean(jnp.square(d), axis=-1, keepdims=True)
            hh = (d * lax.rsqrt(var + EPS) * gf[b]).astype(jnp.bfloat16)
            for k in range(KT):
                h[k, r:r + LR, :] = hh[:, k * T:(k + 1) * T]

    def mm1(n):
        lhs = jnp.concatenate([h[k] for k in range(KT)], axis=1)
        rhs = cols1(n // (NP // 2), n % (NP // 2))
        t = jnp.dot(lhs, rhs, preferred_element_type=jnp.float32)
        for u in range(2):
            a[2 * n + u] = _gelu(t[:, u * T:(u + 1) * T]).astype(jnp.bfloat16)

    def mm2(n, q):
        s, so = lax.rem(q, NS), lax.rem(q, NO)
        lhs = jnp.concatenate([a[k] for k in range(NT)], axis=1)
        rhs = w2v[:2 * FH, 2 * n * T:2 * (n + 1) * T]
        t = jnp.dot(lhs, rhs, preferred_element_type=jnp.float32)
        cols = slice(2 * n * T, 2 * (n + 1) * T)
        ob[so, :, cols] = (ybuf[s, :, cols].astype(jnp.float32) + t).astype(jnp.bfloat16)

    def slot_free(q, ok=True):
        @pl.when(ok & has_next & ((j > 0) | (q >= TP)))
        def _():
            send(q).wait_send()

        @pl.when(ok & odd)
        def _():
            out_local(q).wait()

        if OV:
            @pl.when(ok & odd & whole(q))
            def _():
                tail_local(q).wait()

    def put_out(q, sends):
        pl.semaphore_wait(credit, 1)
        pl.semaphore_signal(credit, 1, device_id=prv, device_id_type=MESH)

        @pl.when(sends)
        def _():
            send(q).start()

        @pl.when(odd & (q < HC))
        def _():
            out_remote(q).start()

        @pl.when(odd & (q >= HC))
        def _():
            out_local(q).start()

        if OV:
            @pl.when(odd & (q < HC) & whole(q))
            def _():
                tail_remote(q).start()

            @pl.when(odd & (q >= HC) & whole(q))
            def _():
                tail_local(q).start()

        @pl.when((j == 0) & (q + LX < HC))
        def _():
            arrival(q + LX).start()

        @pl.when((j == 1) & (q + LX > HC) & (q + LX < NC))
        def _():
            xpush(q + LX - 1).wait_send()

        @pl.when((j == 1) & (q + LX >= HC) & (q + LX < NC))
        def _():
            xpush(q + LX).start()

    def partial(q, b):
        return pltpu.make_async_remote_copy(pb.at[lax.rem(q, 2)], pr.at[lax.rem(q, 2)], ps.at[lax.rem(q, 2)],
                                            prs.at[lax.rem(q, 2) + 2 * b], device_id=partner, device_id_type=MESH)

    def both(q):
        k = lax.rem(q, 2)
        return pb[k].astype(jnp.float32) + pr[k].astype(jnp.float32)

    def split(t, _):
        b, q = lax.rem(lax.div(t, 2), 2), 2 * lax.div(t, 4) + lax.rem(t, 2)
        k, s = lax.rem(q, 2), lax.rem(q, NS)

        @pl.when(t == 0)
        def _():
            own(0)

        @pl.when(t == 2)
        def _():
            own(1)

        @pl.when(b == 0)
        def _():
            arrival(q).wait()

        @pl.when(b == 1)
        def _():
            partial(q, 0).wait_recv()
            ybuf[s] = (ybuf[s].astype(jnp.float32) + both(q)).astype(jnp.bfloat16)

        @pl.when((b == 1) & odd)
        def _():
            pl.semaphore_signal(seen, 1, device_id=partner, device_id_type=MESH)

        @pl.when((b == 1) | ((t >= 4) & (i == 0)))
        def _():
            partial(q, b).wait_send()

        ln(s, b)
        for n in range(NH // 2):
            lhs = jnp.concatenate([h[k2] for k2 in range(KT)], axis=1)
            rhs = cols1(base(b), n)
            u = jnp.dot(lhs, rhs, preferred_element_type=jnp.float32)
            for v in range(2):
                a[2 * n + v] = _gelu(u[:, v * T:(v + 1) * T]).astype(jnp.bfloat16)
        for n in range(N2):
            lhs = jnp.concatenate([a[k2] for k2 in range(NH)], axis=1)
            rhs = w2v[deep(base(b)), 2 * n * T:2 * (n + 1) * T]
            u = jnp.dot(lhs, rhs, preferred_element_type=jnp.float32)
            pb[k, :, 2 * n * T:2 * (n + 1) * T] = u.astype(jnp.bfloat16)

        @pl.when((i == 0) & (lax.rem(t, 4) == 0) & (t >= 4))
        def _():
            pl.semaphore_wait(pair, 1)

        @pl.when((b == 1) & (i == 0))
        def _():
            pl.semaphore_wait(seen, 1)

        @pl.when((b == 0) | (i == 0))
        def _():
            partial(q, b).start()

        @pl.when(t + EARLY < 4)
        def _():
            give1(t + EARLY).start()

        @pl.when((t + EARLY >= 4) & (t + EARLY < 8))
        def _():
            give2(t + EARLY).start()

        @pl.when((b == 1) & odd & (q >= NO))
        def _():
            slot_free(q - NO)

        @pl.when((b == 1) & odd)
        def _():
            partial(q, 1).wait_recv()
            ob[lax.rem(q, NO)] = (ybuf[s].astype(jnp.float32) + both(q)).astype(jnp.bfloat16)

        @pl.when(b == 1)
        def _():
            put_out(q, odd)

        @pl.when(odd & (lax.rem(t, 4) == 3) & (t < 2 * TP - 1))
        def _():
            pl.semaphore_signal(pair, 1, device_id=partner, device_id_type=MESH)
        return 0

    @pl.when(p == 0)
    def _():
        lax.fori_loop(0, 2 * TP, split, 0)

        @pl.when(i == 0)
        def _():
            for q in (TP - 2, TP - 1):
                partial(jnp.int32(q), 1).wait_send()
            pltpu.make_async_copy(x.at[pl.ds(0, TP * C), :], x.at[pl.ds(0, TP * C), :], xs.at[0]).wait()

        @pl.when(odd)
        def _():
            slot_free(jnp.int32(TP - NO))

    @pl.when(p > 0)
    def _():
        own(i)
    got1.wait()
    got2.wait()
    first = jnp.where(p == 0, TP, 0)
    arrival(first).wait()

    def body(q, _):
        ln(lax.rem(q, NS), i)
        for n in range(NP):
            mm1(n)
        for n in range(N2):
            mm2(n, q)
        put_out(q, has_next)

        @pl.when(q + 1 < NC)
        def _():
            arrival(q + 1).wait()
        slot_free(q + 1 - NO, q + 1 >= NO)
        return 0

    lax.fori_loop(first, NC, body, 0)

    for d in range(1, NO):
        slot_free(jnp.int32(NC - NO + d))

    pl.semaphore_wait(credit, NS)

    @pl.when(j == 1)
    def _():
        xpush(jnp.int32(NC - 1)).wait_send()

    sent1.wait()
    sent2.wait()

    @pl.when(i == 0)
    def _():
        pltpu.make_async_copy(y, y, yr.at[0]).wait()


def _move(n, src, dst, buf, isem, osem):
    b = src.shape[0] // n
    into = [pltpu.make_async_copy(src.at[pl.ds(k * b, b), :], buf.at[pl.ds(k * b, b), :], isem.at[k]) for k in range(n)]
    outof = [pltpu.make_async_copy(buf.at[pl.ds(k * b, b), :], dst.at[pl.ds(k * b, b), :], osem.at[k]) for k in range(n)]
    for cp in into:
        cp.start()
    for k in range(n):
        into[k].wait()
        outof[k].start()
    for cp in outof:
        cp.wait()


def solution(mesh):
    S = mesh.shape['stage']

    def local(x, g, w1, w2):
        M, TL, D = x.shape
        FH = w1.shape[-1]
        bf = jnp.bfloat16
        dma = pltpu.SemaphoreType.DMA
        out = pl.pallas_call(
            functools.partial(_kernel, S, M * TL, D, FH),
            out_shape=jax.ShapeDtypeStruct((M * TL, D), bf),
            in_specs=[pl.BlockSpec(memory_space=pl.ANY)] * 4,
            out_specs=pl.BlockSpec(memory_space=pl.ANY),
            scratch_shapes=[
                pltpu.VMEM((3, 2, D, FH // 2), bf),
                pltpu.VMEM((3 * FH, D), bf),
                pltpu.VMEM((2, D), bf),
                pltpu.VMEM((2, 1, D), jnp.float32),
                pltpu.VMEM((NS, C, D), bf),
                pltpu.VMEM((NO, C, D), bf),
                pltpu.VMEM((D // T, C, T), bf),
                pltpu.VMEM((2 * FH // T, C, T), bf),
                pltpu.VMEM((2, C, D), bf),
                pltpu.VMEM((2, C, D), bf),
                dma((NS,)), dma((NO,)), dma((NO,)), dma((NO,)), dma((1,)), dma((1,)),
                dma((4,)), dma((2,)), dma((2,)), dma((1,)), dma((2,)), dma((4,)),
                pltpu.SemaphoreType.REGULAR, pltpu.SemaphoreType.REGULAR, pltpu.SemaphoreType.REGULAR,
            ],
            compiler_params=pltpu.CompilerParams(
                collective_id=0, has_side_effects=True, vmem_limit_bytes=67043328),
            cost_estimate=pl.CostEstimate(flops=8 * M * TL * D * 2 * FH, bytes_accessed=4 * M * TL * D, transcendentals=0),
        )(x.reshape(M * TL, D), g, w1, w2)
        n = 16
        out = pl.pallas_call(
            functools.partial(_move, n),
            out_shape=jax.ShapeDtypeStruct(out.shape, out.dtype),
            in_specs=[pl.BlockSpec(memory_space=pl.ANY)],
            out_specs=pl.BlockSpec(memory_space=pl.ANY),
            scratch_shapes=[pltpu.VMEM(out.shape, out.dtype), dma((n,)), dma((n,))],
            compiler_params=pltpu.CompilerParams(vmem_limit_bytes=67043328),
        )(out)
        return out.reshape(1, M, TL, D)

    return jax.shard_map(
        local, mesh=mesh,
        in_specs=(P(None, 'tp', None), P('stage', None, None),
                  P('stage', None, None, 'tp'), P('stage', None, 'tp', None)),
        out_specs=P('stage', None, 'tp', None), check_vma=False)
```

```python
import functools

import jax
import jax.numpy as jnp
from jax import lax
from jax.experimental import pallas as pl
from jax.experimental.pallas import tpu as pltpu
from jax.sharding import PartitionSpec as P

EPS = 1e-5
C = 144
NS = 4
NO = 3
TP = 4
LR = 24
T = 256
EARLY = 2


def _gelu(u):
    k0 = 0.7978845608028654
    k1 = k0 * 0.044715
    return u * (0.5 + 0.5 * jnp.tanh(u * (k0 + k1 * (u * u))))


def _kernel(S, R, D, FH, x, g, w1, w2, y,
            w1v, w2v, gv, gf, ybuf, ob, h, a, pb, pr,
            rs, ss, osem, otail, yr, xs, wl, wrs, wrr, gs, ps, prs, credit, pair, seen):
    KT, NH = D // T, FH // T
    NT = 2 * NH
    NP, N2 = NT // 2, KT // 2
    NV, W = w1v.shape[1], w1v.shape[3]
    HC = -(-R // C)
    OV = HC * C - R
    NC = 2 * HC
    LX = NS
    B = C - OV

    p = lax.axis_index('stage')
    i = lax.axis_index('tp')
    j = 2 * p + i
    last = 2 * S - 1
    has_prev, has_next = j > 0, j < last
    odd = i == 1
    prv = (lax.rem(p + S - 1 + i, S), 1 - i)
    nxt = (lax.rem(p + i, S), 1 - i)
    partner = (p, 1 - i)
    MESH = pl.DeviceIdType.MESH

    def rows(q, skip=0, n=C):
        r = lax.rem(q, HC)
        at = r * C - lax.div(r, HC - 1) * OV + skip
        return pl.ds(pl.multiple_of(at, 16), n)

    def arrival(q):
        s = lax.rem(q, NS)
        return pltpu.make_async_copy(x.at[rows(q), :], ybuf.at[s], rs.at[s])

    def send(q):
        so, s = lax.rem(q, NO), lax.rem(q, NS)
        return pltpu.make_async_remote_copy(ob.at[so], ybuf.at[s], ss.at[so], rs.at[s], device_id=nxt, device_id_type=MESH)

    def xpush(q):
        s = lax.rem(q, NS)
        return pltpu.make_async_remote_copy(x.at[rows(q), :], ybuf.at[s], xs.at[0], rs.at[s], device_id=prv, device_id_type=MESH)

    def xfeed(q):
        return pltpu.make_async_remote_copy(x.at[rows(q), :], ybuf.at[q], xs.at[0], rs.at[q], device_id=nxt, device_id_type=MESH)

    def out_local(q):
        so = lax.rem(q, NO)
        return pltpu.make_async_copy(ob.at[so, pl.ds(OV, B)], y.at[rows(q, OV, B), :], osem.at[so])

    def out_remote(q):
        so = lax.rem(q, NO)
        return pltpu.make_async_remote_copy(ob.at[so, pl.ds(OV, B)], y.at[rows(q, OV, B), :], osem.at[so], yr.at[0],
                                            device_id=partner, device_id_type=MESH)

    def tail_local(q):
        so = lax.rem(q, NO)
        return pltpu.make_async_copy(ob.at[so, pl.ds(0, OV)], y.at[rows(q, 0, OV), :], otail.at[so])

    def tail_remote(q):
        so = lax.rem(q, NO)
        return pltpu.make_async_remote_copy(ob.at[so, pl.ds(0, OV)], y.at[rows(q, 0, OV), :], otail.at[so], yr.at[0],
                                            device_id=partner, device_id_type=MESH)

    def whole(q):
        return lax.rem(q, HC) < HC - 1

    def base(b):
        return 2 * lax.rem(b + i, 2)

    def deep(third):
        return pl.ds(pl.multiple_of(third * FH, T), FH)

    def load(b):
        r1, r2 = D // 2, FH // 4
        return [pltpu.make_async_copy(w1.at[0, b, pl.ds(r * r1, r1), pl.ds(v * W, W)], w1v.at[base(b), v, pl.ds(r * r1, r1), :], wl.at[b])
                for v in range(NV) for r in range(2)] + [
            pltpu.make_async_copy(w2.at[0, b, pl.ds(r * r2, r2), :],
                                  w2v.at[pl.ds(pl.multiple_of(base(b) * FH + r * r2, 16), r2), :], wl.at[2 + b]) for r in range(4)]

    D4, F4 = D // (4 // NV), FH // 4

    def give1(t):
        at = lax.rem(t, 4 // NV), lax.div(t, 4 // NV)
        r, v = pl.ds(pl.multiple_of(at[0] * D4, 16), D4), at[1]
        return pltpu.make_async_remote_copy(w1.at[0, 1 - i, r, pl.ds(pl.multiple_of(v * W, T), W)], w1v.at[1, v, r, :],
                                            wrs.at[0], wrr.at[0], device_id=partner, device_id_type=MESH)

    def give2(t):
        r = lax.rem(t, 4) * F4
        return pltpu.make_async_remote_copy(w2.at[0, 1 - i, pl.ds(pl.multiple_of(r, 16), F4), :],
                                            w2v.at[pl.ds(pl.multiple_of(FH + r, 16), F4), :],
                                            wrs.at[1], wrr.at[1], device_id=partner, device_id_type=MESH)

    half1, half2 = w1v.at[1], w2v.at[pl.ds(0, FH), :]
    got1, sent1 = (pltpu.make_async_copy(half1, half1, sem) for sem in (wrr.at[0], wrs.at[0]))
    got2, sent2 = (pltpu.make_async_copy(half2, half2, sem) for sem in (wrr.at[1], wrs.at[1]))

    def own1(b):
        pltpu.make_async_copy(half1, half1, wl.at[b]).wait()

    def own2(b):
        pltpu.make_async_copy(half2, half2, wl.at[2 + b]).wait()

    def own(b):
        own1(b)
        own2(b)

    def cols1(third, n):
        v, at = divmod(2 * n * T, W)
        return w1v[third, v, :, at:at + 2 * T]

    gcopy = pltpu.make_async_copy(g.at[0], gv, gs.at[0])

    bar = pltpu.get_barrier_semaphore()

    @pl.when(has_prev)
    def _():
        pl.semaphore_signal(bar, 1, device_id=prv, device_id_type=MESH)

    @pl.when(has_next)
    def _():
        pl.semaphore_signal(bar, 1, device_id=nxt, device_id_type=MESH)

    gcopy.start()

    @pl.when(j == 0)
    def _():
        for q in range(LX):
            arrival(q).start()

    for b in range(2):
        @pl.when((i == b) & (p > 0) if b else (p == 0) | (i == b))
        def _():
            for cp in load(b):
                cp.start()

    @pl.when(has_prev & has_next)
    def _():
        pl.semaphore_wait(bar, 2)

    @pl.when((j == 0) | (j == last))
    def _():
        pl.semaphore_wait(bar, 1)

    @pl.when(j == 0)
    def _():
        for q in range(TP):
            xfeed(q).start()

    for t in range(EARLY):
        give1(jnp.int32(t)).start()

    @pl.when(p > 0)
    def _():
        for t in range(EARLY, 4):
            give1(jnp.int32(t)).start()
        for t in range(4):
            give2(jnp.int32(t)).start()

    @pl.when(has_prev)
    def _():
        pl.semaphore_signal(credit, NS, device_id=prv, device_id_type=MESH)


    gcopy.wait()
    for b in range(2):
        gf[b] = gv[b:b + 1, :].astype(jnp.float32)

    def ln(s, b):
        for r in range(0, C, LR):
            yf = ybuf[s, r:r + LR, :].astype(jnp.float32)
            mu = jnp.mean(yf, axis=-1, keepdims=True)
            d = yf - mu
            var = jnp.mean(jnp.square(d), axis=-1, keepdims=True)
            hh = (d * lax.rsqrt(var + EPS) * gf[b]).astype(jnp.bfloat16)
            for k in range(KT):
                h[k, r:r + LR, :] = hh[:, k * T:(k + 1) * T]

    def mm1(n):
        lhs = jnp.concatenate([h[k] for k in range(KT)], axis=1)
        rhs = cols1(n // (NP // 2), n % (NP // 2))
        t = jnp.dot(lhs, rhs, preferred_element_type=jnp.float32)
        for u in range(2):
            a[2 * n + u] = _gelu(t[:, u * T:(u + 1) * T]).astype(jnp.bfloat16)

    def mm2(n, q):
        s, so = lax.rem(q, NS), lax.rem(q, NO)
        lhs = jnp.concatenate([a[k] for k in range(NT)], axis=1)
        rhs = w2v[:2 * FH, 2 * n * T:2 * (n + 1) * T]
        t = jnp.dot(lhs, rhs, preferred_element_type=jnp.float32)
        cols = slice(2 * n * T, 2 * (n + 1) * T)
        ob[so, :, cols] = (ybuf[s, :, cols].astype(jnp.float32) + t).astype(jnp.bfloat16)

    def slot_free(q, ok=True):
        @pl.when(ok & has_next & ((j > 0) | (q >= TP)))
        def _():
            send(q).wait_send()

        @pl.when(ok & odd)
        def _():
            out_local(q).wait()

        if OV:
            @pl.when(ok & odd & whole(q))
            def _():
                tail_local(q).wait()

    def put_out(q, sends):
        @pl.when(has_next)
        def _():
            pl.semaphore_wait(credit, 1)

        @pl.when(has_prev)
        def _():
            pl.semaphore_signal(credit, 1, device_id=prv, device_id_type=MESH)

        @pl.when(sends)
        def _():
            send(q).start()

        @pl.when(odd & (q < HC))
        def _():
            out_remote(q).start()

        @pl.when(odd & (q >= HC))
        def _():
            out_local(q).start()

        if OV:
            @pl.when(odd & (q < HC) & whole(q))
            def _():
                tail_remote(q).start()

            @pl.when(odd & (q >= HC) & whole(q))
            def _():
                tail_local(q).start()

        @pl.when((j == 0) & (q + LX < HC))
        def _():
            arrival(q + LX).start()

        @pl.when((j == 1) & (q + LX > HC) & (q + LX < NC))
        def _():
            xpush(q + LX - 1).wait_send()

        @pl.when((j == 1) & (q + LX >= HC) & (q + LX < NC))
        def _():
            xpush(q + LX).start()

    def partial(q, b):
        return pltpu.make_async_remote_copy(pb.at[lax.rem(q, 2)], pr.at[lax.rem(q, 2)], ps.at[lax.rem(q, 2)],
                                            prs.at[lax.rem(q, 2) + 2 * b], device_id=partner, device_id_type=MESH)

    def both(q):
        k = lax.rem(q, 2)
        return pb[k].astype(jnp.float32) + pr[k].astype(jnp.float32)

    def split(t, _):
        b, q = lax.rem(lax.div(t, 2), 2), 2 * lax.div(t, 4) + lax.rem(t, 2)
        k, s = lax.rem(q, 2), lax.rem(q, NS)

        @pl.when(t == 0)
        def _():
            own(0)
            for cp in load(1):
                cp.start()

        @pl.when(t == 2)
        def _():
            own(1)

        @pl.when(b == 0)
        def _():
            arrival(q).wait()

        @pl.when(b == 1)
        def _():
            partial(q, 0).wait_recv()
            ybuf[s] = (ybuf[s].astype(jnp.float32) + both(q)).astype(jnp.bfloat16)

        @pl.when((b == 1) & odd)
        def _():
            pl.semaphore_signal(seen, 1, device_id=partner, device_id_type=MESH)

        @pl.when((b == 1) | ((t >= 4) & (i == 0)))
        def _():
            partial(q, b).wait_send()

        ln(s, b)
        for n in range(NH // 2):
            lhs = jnp.concatenate([h[k2] for k2 in range(KT)], axis=1)
            rhs = cols1(base(b), n)
            u = jnp.dot(lhs, rhs, preferred_element_type=jnp.float32)
            for v in range(2):
                a[2 * n + v] = _gelu(u[:, v * T:(v + 1) * T]).astype(jnp.bfloat16)
        for n in range(N2):
            lhs = jnp.concatenate([a[k2] for k2 in range(NH)], axis=1)
            rhs = w2v[deep(base(b)), 2 * n * T:2 * (n + 1) * T]
            u = jnp.dot(lhs, rhs, preferred_element_type=jnp.float32)
            pb[k, :, 2 * n * T:2 * (n + 1) * T] = u.astype(jnp.bfloat16)

        @pl.when((i == 0) & (lax.rem(t, 4) == 0) & (t >= 4))
        def _():
            pl.semaphore_wait(pair, 1)

        @pl.when((b == 1) & (i == 0))
        def _():
            pl.semaphore_wait(seen, 1)

        @pl.when((b == 0) | (i == 0))
        def _():
            partial(q, b).start()

        @pl.when(t + EARLY < 4)
        def _():
            give1(t + EARLY).start()

        @pl.when((t + EARLY >= 4) & (t + EARLY < 8))
        def _():
            give2(t + EARLY).start()

        def go_out(q):
            slot_free(q - NO, odd & (q >= NO))

            @pl.when(odd)
            def _():
                partial(q, 1).wait_recv()
                ob[lax.rem(q, NO)] = (ybuf[lax.rem(q, NS)].astype(jnp.float32) + both(q)).astype(jnp.bfloat16)
            put_out(q, odd)

        @pl.when(lax.rem(t, 4) == 3)
        def _():
            go_out(q - 1)
            go_out(q)

        @pl.when(odd & (lax.rem(t, 4) == 3) & (t < 2 * TP - 1))
        def _():
            pl.semaphore_signal(pair, 1, device_id=partner, device_id_type=MESH)
        return 0

    @pl.when(p == 0)
    def _():
        lax.fori_loop(0, 2 * TP, split, 0)

        @pl.when(i == 0)
        def _():
            for q in (TP - 2, TP - 1):
                partial(jnp.int32(q), 1).wait_send()
            pltpu.make_async_copy(x.at[pl.ds(0, TP * C), :], x.at[pl.ds(0, TP * C), :], xs.at[0]).wait()

        @pl.when(odd)
        def _():
            slot_free(jnp.int32(TP - NO))

    @pl.when(p > 0)
    def _():
        own(i)
    got1.wait()
    got2.wait()
    first = jnp.where(p == 0, TP, 0)
    arrival(first).wait()

    def body(q, _):
        ln(lax.rem(q, NS), i)
        for n in range(NP):
            mm1(n)
        for n in range(N2):
            mm2(n, q)
        put_out(q, has_next)

        @pl.when(q + 1 < NC)
        def _():
            arrival(q + 1).wait()
        slot_free(q + 1 - NO, q + 1 >= NO)
        return 0

    lax.fori_loop(first, NC, body, 0)

    for d in range(1, NO):
        slot_free(jnp.int32(NC - NO + d))

    @pl.when(has_next)
    def _():
        pl.semaphore_wait(credit, NS)

    @pl.when(j == 1)
    def _():
        xpush(jnp.int32(NC - 1)).wait_send()

    sent1.wait()
    sent2.wait()

    @pl.when(i == 0)
    def _():
        pltpu.make_async_copy(y, y, yr.at[0]).wait()


def _move(n, src, dst, buf, isem, osem):
    b = src.shape[0] // n
    into = [pltpu.make_async_copy(src.at[pl.ds(k * b, b), :], buf.at[pl.ds(k * b, b), :], isem.at[k]) for k in range(n)]
    outof = [pltpu.make_async_copy(buf.at[pl.ds(k * b, b), :], dst.at[pl.ds(k * b, b), :], osem.at[k]) for k in range(n)]
    for cp in into:
        cp.start()
    for k in range(n):
        into[k].wait()
        outof[k].start()
    for cp in outof:
        cp.wait()


def solution(mesh):
    S = mesh.shape['stage']

    def local(x, g, w1, w2):
        M, TL, D = x.shape
        FH = w1.shape[-1]
        bf = jnp.bfloat16
        dma = pltpu.SemaphoreType.DMA
        out = pl.pallas_call(
            functools.partial(_kernel, S, M * TL, D, FH),
            out_shape=jax.ShapeDtypeStruct((M * TL, D), bf),
            in_specs=[pl.BlockSpec(memory_space=pl.ANY)] * 4,
            out_specs=pl.BlockSpec(memory_space=pl.ANY),
            scratch_shapes=[
                pltpu.VMEM((3, 2, D, FH // 2), bf),
                pltpu.VMEM((3 * FH, D), bf),
                pltpu.VMEM((2, D), bf),
                pltpu.VMEM((2, 1, D), jnp.float32),
                pltpu.VMEM((NS, C, D), bf),
                pltpu.VMEM((NO, C, D), bf),
                pltpu.VMEM((D // T, C, T), bf),
                pltpu.VMEM((2 * FH // T, C, T), bf),
                pltpu.VMEM((2, C, D), bf),
                pltpu.VMEM((2, C, D), bf),
                dma((NS,)), dma((NO,)), dma((NO,)), dma((NO,)), dma((1,)), dma((1,)),
                dma((4,)), dma((2,)), dma((2,)), dma((1,)), dma((2,)), dma((4,)),
                pltpu.SemaphoreType.REGULAR, pltpu.SemaphoreType.REGULAR, pltpu.SemaphoreType.REGULAR,
            ],
            compiler_params=pltpu.CompilerParams(
                collective_id=0, has_side_effects=True, vmem_limit_bytes=67043328),
            cost_estimate=pl.CostEstimate(flops=8 * M * TL * D * 2 * FH, bytes_accessed=4 * M * TL * D, transcendentals=0),
        )(x.reshape(M * TL, D), g, w1, w2)
        n = 16
        out = pl.pallas_call(
            functools.partial(_move, n),
            out_shape=jax.ShapeDtypeStruct(out.shape, out.dtype),
            in_specs=[pl.BlockSpec(memory_space=pl.ANY)],
            out_specs=pl.BlockSpec(memory_space=pl.ANY),
            scratch_shapes=[pltpu.VMEM(out.shape, out.dtype), dma((n,)), dma((n,))],
            compiler_params=pltpu.CompilerParams(vmem_limit_bytes=67043328),
        )(out)
        return out.reshape(1, M, TL, D)

    return jax.shard_map(
        local, mesh=mesh,
        in_specs=(P(None, 'tp', None), P('stage', None, None),
                  P('stage', None, None, 'tp'), P('stage', None, 'tp', None)),
        out_specs=P('stage', None, 'tp', None), check_vma=False)
```

```python
import functools

import jax
import jax.numpy as jnp
from jax import lax
from jax.experimental import pallas as pl
from jax.experimental.pallas import tpu as pltpu
from jax.sharding import PartitionSpec as P

EPS = 1e-5
C = 144
NS = 4
NO = 3
TP = 4
LR = 24
T = 256
EARLY = 2


def _gelu(u):
    k0 = 0.7978845608028654
    k1 = k0 * 0.044715
    return u * (0.5 + 0.5 * jnp.tanh(u * (k0 + k1 * (u * u))))


def _kernel(S, R, D, FH, x, g, w1, w2, y,
            w1v, w2v, gv, gf, ybuf, ob, h, a, pb, pr,
            rs, ss, osem, otail, yr, xs, wl, wrs, wrr, gs, ps, prs, credit, pair, seen):
    KT, NH = D // T, FH // T
    NT = 2 * NH
    NP, N2 = NT // 2, KT // 2
    NV, W = w1v.shape[1], w1v.shape[3]
    HC = -(-R // C)
    OV = HC * C - R
    NC = 2 * HC
    LX = NS
    B = C - OV

    p = lax.axis_index('stage')
    i = lax.axis_index('tp')
    j = 2 * p + i
    last = 2 * S - 1
    has_prev, has_next = j > 0, j < last
    odd = i == 1
    prv = (lax.rem(p + S - 1 + i, S), 1 - i)
    nxt = (lax.rem(p + i, S), 1 - i)
    partner = (p, 1 - i)
    MESH = pl.DeviceIdType.MESH

    def rows(q, skip=0, n=C):
        r = lax.rem(q, HC)
        at = r * C - lax.div(r, HC - 1) * OV + skip
        return pl.ds(pl.multiple_of(at, 16), n)

    def arrival(q):
        s = lax.rem(q, NS)
        return pltpu.make_async_copy(x.at[rows(q), :], ybuf.at[s], rs.at[s])

    def send(q):
        so, s = lax.rem(q, NO), lax.rem(q, NS)
        return pltpu.make_async_remote_copy(ob.at[so], ybuf.at[s], ss.at[so], rs.at[s], device_id=nxt, device_id_type=MESH)

    def xpush(q):
        s = lax.rem(q, NS)
        return pltpu.make_async_remote_copy(x.at[rows(q), :], ybuf.at[s], xs.at[0], rs.at[s], device_id=prv, device_id_type=MESH)

    def xfeed(q):
        return pltpu.make_async_remote_copy(x.at[rows(q), :], ybuf.at[q], xs.at[0], rs.at[q], device_id=nxt, device_id_type=MESH)

    def out_local(q):
        so = lax.rem(q, NO)
        return pltpu.make_async_copy(ob.at[so, pl.ds(OV, B)], y.at[rows(q, OV, B), :], osem.at[so])

    def out_remote(q):
        so = lax.rem(q, NO)
        return pltpu.make_async_remote_copy(ob.at[so, pl.ds(OV, B)], y.at[rows(q, OV, B), :], osem.at[so], yr.at[0],
                                            device_id=partner, device_id_type=MESH)

    def tail_local(q):
        so = lax.rem(q, NO)
        return pltpu.make_async_copy(ob.at[so, pl.ds(0, OV)], y.at[rows(q, 0, OV), :], otail.at[so])

    def tail_remote(q):
        so = lax.rem(q, NO)
        return pltpu.make_async_remote_copy(ob.at[so, pl.ds(0, OV)], y.at[rows(q, 0, OV), :], otail.at[so], yr.at[0],
                                            device_id=partner, device_id_type=MESH)

    def whole(q):
        return lax.rem(q, HC) < HC - 1

    def base(b):
        return 2 * lax.rem(b + i, 2)

    def deep(third):
        return pl.ds(pl.multiple_of(third * FH, T), FH)

    def load(b):
        r1, r2 = D // 2, FH // 4
        return [pltpu.make_async_copy(w1.at[0, b, pl.ds(r * r1, r1), pl.ds(v * W, W)], w1v.at[base(b), v, pl.ds(r * r1, r1), :], wl.at[b])
                for v in range(NV) for r in range(2)] + [
            pltpu.make_async_copy(w2.at[0, b, pl.ds(r * r2, r2), :],
                                  w2v.at[pl.ds(pl.multiple_of(base(b) * FH + r * r2, 16), r2), :], wl.at[2 + b]) for r in range(4)]

    D4, F4 = D // (4 // NV), FH // 4

    def give1(t):
        at = lax.rem(t, 4 // NV), lax.div(t, 4 // NV)
        r, v = pl.ds(pl.multiple_of(at[0] * D4, 16), D4), at[1]
        return pltpu.make_async_remote_copy(w1.at[0, 1 - i, r, pl.ds(pl.multiple_of(v * W, T), W)], w1v.at[1, v, r, :],
                                            wrs.at[0], wrr.at[0], device_id=partner, device_id_type=MESH)

    def give2(t):
        r = lax.rem(t, 4) * F4
        return pltpu.make_async_remote_copy(w2.at[0, 1 - i, pl.ds(pl.multiple_of(r, 16), F4), :],
                                            w2v.at[pl.ds(pl.multiple_of(FH + r, 16), F4), :],
                                            wrs.at[1], wrr.at[1], device_id=partner, device_id_type=MESH)

    half1, half2 = w1v.at[1], w2v.at[pl.ds(0, FH), :]
    got1, sent1 = (pltpu.make_async_copy(half1, half1, sem) for sem in (wrr.at[0], wrs.at[0]))
    got2, sent2 = (pltpu.make_async_copy(half2, half2, sem) for sem in (wrr.at[1], wrs.at[1]))

    def own1(b):
        pltpu.make_async_copy(half1, half1, wl.at[b]).wait()

    def own2(b):
        pltpu.make_async_copy(half2, half2, wl.at[2 + b]).wait()

    def own(b):
        own1(b)
        own2(b)

    def cols1(third, n):
        v, at = divmod(2 * n * T, W)
        return w1v[third, v, :, at:at + 2 * T]

    gcopy = pltpu.make_async_copy(g.at[0], gv, gs.at[0])

    bar = pltpu.get_barrier_semaphore()

    @pl.when(has_prev)
    def _():
        pl.semaphore_signal(bar, 1, device_id=prv, device_id_type=MESH)

    @pl.when(has_next)
    def _():
        pl.semaphore_signal(bar, 1, device_id=nxt, device_id_type=MESH)

    gcopy.start()

    @pl.when(j == 0)
    def _():
        for q in range(LX):
            arrival(q).start()

    for b in range(2):
        @pl.when((i == b) & (p > 0) if b else (p == 0) | (i == b))
        def _():
            for cp in load(b):
                cp.start()

    @pl.when(has_prev & has_next)
    def _():
        pl.semaphore_wait(bar, 2)

    @pl.when((j == 0) | (j == last))
    def _():
        pl.semaphore_wait(bar, 1)

    @pl.when(j == 0)
    def _():
        for q in range(TP):
            xfeed(q).start()

    for t in range(EARLY):
        give1(jnp.int32(t)).start()

    @pl.when(p > 0)
    def _():
        for t in range(EARLY, 4):
            give1(jnp.int32(t)).start()
        for t in range(4):
            give2(jnp.int32(t)).start()

    @pl.when(has_prev)
    def _():
        pl.semaphore_signal(credit, NS, device_id=prv, device_id_type=MESH)


    gcopy.wait()
    for b in range(2):
        gf[b] = gv[b:b + 1, :].astype(jnp.float32)

    def ln(s, b):
        for r in range(0, C, LR):
            yf = ybuf[s, r:r + LR, :].astype(jnp.float32)
            mu = jnp.mean(yf, axis=-1, keepdims=True)
            d = yf - mu
            var = jnp.mean(jnp.square(d), axis=-1, keepdims=True)
            hh = (d * lax.rsqrt(var + EPS) * gf[b]).astype(jnp.bfloat16)
            for k in range(KT):
                h[k, r:r + LR, :] = hh[:, k * T:(k + 1) * T]

    def mm1(n):
        lhs = jnp.concatenate([h[k] for k in range(KT)], axis=1)
        rhs = cols1(n // (NP // 2), n % (NP // 2))
        t = jnp.dot(lhs, rhs, preferred_element_type=jnp.float32)
        for u in range(2):
            a[2 * n + u] = _gelu(t[:, u * T:(u + 1) * T]).astype(jnp.bfloat16)

    def mm2(n, q):
        s, so = lax.rem(q, NS), lax.rem(q, NO)
        lhs = jnp.concatenate([a[k] for k in range(NT)], axis=1)
        rhs = w2v[:2 * FH, 2 * n * T:2 * (n + 1) * T]
        t = jnp.dot(lhs, rhs, preferred_element_type=jnp.float32)
        cols = slice(2 * n * T, 2 * (n + 1) * T)
        ob[so, :, cols] = (ybuf[s, :, cols].astype(jnp.float32) + t).astype(jnp.bfloat16)

    def slot_free(q, ok=True):
        @pl.when(ok & has_next & ((j > 0) | (q >= TP)))
        def _():
            send(q).wait_send()

        @pl.when(ok & odd)
        def _():
            out_local(q).wait()

        if OV:
            @pl.when(ok & odd & whole(q))
            def _():
                tail_local(q).wait()

    def put_out(q, sends, half):
        @pl.when(has_next)
        def _():
            pl.semaphore_wait(credit, 1)

            if sends is True:
                send(q).start()
            else:
                @pl.when(sends)
                def _():
                    send(q).start()

        @pl.when(has_prev)
        def _():
            pl.semaphore_signal(credit, 1, device_id=prv, device_id_type=MESH)

        @pl.when(odd)
        def _():
            (out_local if half else out_remote)(q).start()

        if OV:
            @pl.when(odd & whole(q))
            def _():
                (tail_local if half else tail_remote)(q).start()

        if not half:
            @pl.when((j == 0) & (q + LX < HC))
            def _():
                arrival(q + LX).start()

        @pl.when((j == 1) & (q + LX > HC) & (q + LX < NC))
        def _():
            xpush(q + LX - 1).wait_send()

        @pl.when((j == 1) & (q + LX >= HC) & (q + LX < NC))
        def _():
            xpush(q + LX).start()

    def partial(q, b):
        return pltpu.make_async_remote_copy(pb.at[lax.rem(q, 2)], pr.at[lax.rem(q, 2)], ps.at[lax.rem(q, 2)],
                                            prs.at[lax.rem(q, 2) + 2 * b], device_id=partner, device_id_type=MESH)

    def both(q):
        k = lax.rem(q, 2)
        return pb[k].astype(jnp.float32) + pr[k].astype(jnp.float32)

    def split(t, _):
        b, q = lax.rem(lax.div(t, 2), 2), 2 * lax.div(t, 4) + lax.rem(t, 2)
        k, s = lax.rem(q, 2), lax.rem(q, NS)

        @pl.when(t == 0)
        def _():
            own(0)
            for cp in load(1):
                cp.start()

        @pl.when(t == 2)
        def _():
            own(1)

        @pl.when(b == 0)
        def _():
            arrival(q).wait()

        @pl.when(b == 1)
        def _():
            partial(q, 0).wait_recv()
            ybuf[s] = (ybuf[s].astype(jnp.float32) + both(q)).astype(jnp.bfloat16)

        @pl.when((b == 1) & odd)
        def _():
            pl.semaphore_signal(seen, 1, device_id=partner, device_id_type=MESH)

        @pl.when((b == 1) | ((t >= 4) & (i == 0)))
        def _():
            partial(q, b).wait_send()

        ln(s, b)
        for n in range(NH // 2):
            lhs = jnp.concatenate([h[k2] for k2 in range(KT)], axis=1)
            rhs = cols1(base(b), n)
            u = jnp.dot(lhs, rhs, preferred_element_type=jnp.float32)
            for v in range(2):
                a[2 * n + v] = _gelu(u[:, v * T:(v + 1) * T]).astype(jnp.bfloat16)
        for n in range(N2):
            lhs = jnp.concatenate([a[k2] for k2 in range(NH)], axis=1)
            rhs = w2v[deep(base(b)), 2 * n * T:2 * (n + 1) * T]
            u = jnp.dot(lhs, rhs, preferred_element_type=jnp.float32)
            pb[k, :, 2 * n * T:2 * (n + 1) * T] = u.astype(jnp.bfloat16)

        @pl.when((i == 0) & (lax.rem(t, 4) == 0) & (t >= 4))
        def _():
            pl.semaphore_wait(pair, 1)

        @pl.when((b == 1) & (i == 0))
        def _():
            pl.semaphore_wait(seen, 1)

        @pl.when((b == 0) | (i == 0))
        def _():
            partial(q, b).start()

        @pl.when(t + EARLY < 4)
        def _():
            give1(t + EARLY).start()

        @pl.when((t + EARLY >= 4) & (t + EARLY < 8))
        def _():
            give2(t + EARLY).start()

        def go_out(q):
            slot_free(q - NO, odd & (q >= NO))

            @pl.when(odd)
            def _():
                partial(q, 1).wait_recv()
                ob[lax.rem(q, NO)] = (ybuf[lax.rem(q, NS)].astype(jnp.float32) + both(q)).astype(jnp.bfloat16)
            put_out(q, odd, 0)

        @pl.when(lax.rem(t, 4) == 3)
        def _():
            go_out(q - 1)
            go_out(q)

        @pl.when(odd & (lax.rem(t, 4) == 3) & (t < 2 * TP - 1))
        def _():
            pl.semaphore_signal(pair, 1, device_id=partner, device_id_type=MESH)
        return 0

    @pl.when(p == 0)
    def _():
        lax.fori_loop(0, 2 * TP, split, 0)

        @pl.when(i == 0)
        def _():
            for q in (TP - 2, TP - 1):
                partial(jnp.int32(q), 1).wait_send()
            pltpu.make_async_copy(x.at[pl.ds(0, TP * C), :], x.at[pl.ds(0, TP * C), :], xs.at[0]).wait()

        @pl.when(odd)
        def _():
            slot_free(jnp.int32(TP - NO))

    @pl.when(p > 0)
    def _():
        own(i)
    got1.wait()
    got2.wait()
    first = jnp.where(p == 0, TP, 0)
    arrival(first).wait()

    def body(half, q, _):
        ln(lax.rem(q, NS), i)
        for n in range(NP):
            mm1(n)
        for n in range(N2):
            mm2(n, q)
        put_out(q, True, half)

        @pl.when(q + 1 < NC)
        def _():
            arrival(q + 1).wait()
        slot_free(q + 1 - NO, q + 1 >= NO)
        return 0

    lax.fori_loop(first, min(HC, NC), functools.partial(body, 0), 0)
    lax.fori_loop(HC, max(HC, NC), functools.partial(body, 1), 0)

    for d in range(1, NO):
        slot_free(jnp.int32(NC - NO + d))

    @pl.when(has_next)
    def _():
        pl.semaphore_wait(credit, NS)

    @pl.when(j == 1)
    def _():
        xpush(jnp.int32(NC - 1)).wait_send()

    sent1.wait()
    sent2.wait()

    @pl.when(i == 0)
    def _():
        pltpu.make_async_copy(y, y, yr.at[0]).wait()


def _move(n, src, dst, buf, isem, osem):
    b = src.shape[0] // n
    into = [pltpu.make_async_copy(src.at[pl.ds(k * b, b), :], buf.at[pl.ds(k * b, b), :], isem.at[k]) for k in range(n)]
    outof = [pltpu.make_async_copy(buf.at[pl.ds(k * b, b), :], dst.at[pl.ds(k * b, b), :], osem.at[k]) for k in range(n)]
    for cp in into:
        cp.start()
    for k in range(n):
        into[k].wait()
    for k in range(n):
        outof[k].start()
    for cp in outof:
        cp.wait()


def solution(mesh):
    S = mesh.shape['stage']

    def local(x, g, w1, w2):
        M, TL, D = x.shape
        FH = w1.shape[-1]
        bf = jnp.bfloat16
        dma = pltpu.SemaphoreType.DMA
        out = pl.pallas_call(
            functools.partial(_kernel, S, M * TL, D, FH),
            out_shape=jax.ShapeDtypeStruct((M * TL, D), bf),
            in_specs=[pl.BlockSpec(memory_space=pl.ANY)] * 4,
            out_specs=pl.BlockSpec(memory_space=pl.ANY),
            scratch_shapes=[
                pltpu.VMEM((3, 2, D, FH // 2), bf),
                pltpu.VMEM((3 * FH, D), bf),
                pltpu.VMEM((2, D), bf),
                pltpu.VMEM((2, 1, D), jnp.float32),
                pltpu.VMEM((NS, C, D), bf),
                pltpu.VMEM((NO, C, D), bf),
                pltpu.VMEM((D // T, C, T), bf),
                pltpu.VMEM((2 * FH // T, C, T), bf),
                pltpu.VMEM((2, C, D), bf),
                pltpu.VMEM((2, C, D), bf),
                dma((NS,)), dma((NO,)), dma((NO,)), dma((NO,)), dma((1,)), dma((1,)),
                dma((4,)), dma((2,)), dma((2,)), dma((1,)), dma((2,)), dma((4,)),
                pltpu.SemaphoreType.REGULAR, pltpu.SemaphoreType.REGULAR, pltpu.SemaphoreType.REGULAR,
            ],
            compiler_params=pltpu.CompilerParams(
                collective_id=0, has_side_effects=True, vmem_limit_bytes=67043328),
            cost_estimate=pl.CostEstimate(flops=8 * M * TL * D * 2 * FH, bytes_accessed=4 * M * TL * D, transcendentals=0),
        )(x.reshape(M * TL, D), g, w1, w2)
        n = 8
        out = pl.pallas_call(
            functools.partial(_move, n),
            out_shape=jax.ShapeDtypeStruct(out.shape, out.dtype),
            in_specs=[pl.BlockSpec(memory_space=pl.ANY)],
            out_specs=pl.BlockSpec(memory_space=pl.ANY),
            scratch_shapes=[pltpu.VMEM(out.shape, out.dtype), dma((n,)), dma((n,))],
            compiler_params=pltpu.CompilerParams(vmem_limit_bytes=67043328),
        )(out)
        return out.reshape(1, M, TL, D)

    return jax.shard_map(
        local, mesh=mesh,
        in_specs=(P(None, 'tp', None), P('stage', None, None),
                  P('stage', None, None, 'tp'), P('stage', None, 'tp', None)),
        out_specs=P('stage', None, 'tp', None), check_vma=False)
```
